32 devices in a mesh: gx: 4 (over y, core), gy: 8 (over z, x).
Axes of the slice: x: 2, y: 2, z: 4, core: 2. Of those that a mesh axis runs over, the one named last changes fastest.
Arguments:
- source: float32 [64, 16, 1024], P(None, 'gx', 'gy'), may hold values from -6 to 6
- initial: float32 [64, 16, 1024], P(None, 'gx', 'gy'), may hold values from -6 to 6
- reaction: float32 [64, 16, 1024], P(None, 'gx', 'gy'), may hold values from 1 to 3
- stiffness: float32 [16, 1024], P('gx', 'gy'), may hold values from 0.5 to 2
- line_op: float32 [8, 8], replicated, may hold values from -1.6 to 5.6
- face_deriv: float32 [8], replicated, may hold values from -2 to 2
- wall_flags: int32 [4, 16, 1024], P(None, 'gx', 'gy'), may hold values 0 or 1
Outputs:
- hessenberg: float32 [6, 5], replicated
- krylov_basis: float32 [6, 64, 16, 1024], P(None, None, 'gx', 'gy')
The draws below stay inside these ranges and needn't reach their ends.
All inputs are finite; a program needn't handle non-finite values. No bound on the sum of `wall_flags` on one device may be relied on, other than what follows from the above.
Results may differ from the reference program's by a relative error of at most 0.0003.
Values sent between devices are 32-bit elements; how exact they have to be, the bound alone decides.
A program may use at most 64 MiB of HBM per device.

```python
import math
import jax
import jax.numpy as jnp
from jax import lax

P_SIZE = 8
ITERS = 5
NEX = 16
NEY = 1024


def draw_line_op(key, part):
    first_key, second_key = jax.random.split(jax.random.fold_in(key, 11))
    offdiag = jnp.clip(jax.random.normal(first_key, (P_SIZE, P_SIZE), jnp.float32) * 0.4, -1.6, 1.6)
    diagonal = jax.random.uniform(second_key, (P_SIZE,), jnp.float32, 2.0, 4.0)
    return offdiag * (1.0 - jnp.eye(P_SIZE, dtype=jnp.float32)) + jnp.diag(diagonal)


def place_ends(values, rng, least, largest):
    longest = values.shape.index(max(values.shape))
    spots = []
    for shift in (0, 1):
        where = [jax.random.randint(jax.random.fold_in(rng, axis), (), 0, length) for axis, length in enumerate(values.shape)]
        where[longest] = (where[longest] + shift) % values.shape[longest]
        spots.append(tuple(where))
    return values.at[spots[0]].set(least).at[spots[1]].set(largest)


def block_scale(rng, extent, cuts, low, largest):
    def one(position, shards_of):
        draws = jax.random.uniform(jax.random.fold_in(jax.random.fold_in(rng, 6), position), (shards_of,), jnp.float32, low / len(cuts), largest / len(cuts))
        return jnp.repeat(jnp.exp(draws), extent[position] // shards_of).reshape((-1,) + (1,) * (len(extent) - position - 1))

    factor_of = one(*cuts[0])
    for cut in cuts[1:]:
        factor_of = factor_of * one(*cut)
    return factor_of


def gaussian(rng, extent, deviation, most, cuts=(), held_as=jnp.bfloat16):
    values = deviation * jax.random.normal(rng, extent, jnp.float32)
    if cuts:
        values = values * block_scale(rng, extent, cuts, -0.22, 0.18)
    return jnp.clip(values, -most, most).astype(held_as)


def setup_inputs(seed: int = 0) -> dict:
    streams_of = jax.random.split(jax.random.key(seed), 8)
    source = gaussian(streams_of[0], (P_SIZE * P_SIZE, NEX, NEY), 1.0, 6.0, ((1, 4), (2, 8)), jnp.float32)
    initial = gaussian(streams_of[1], (P_SIZE * P_SIZE, NEX, NEY), 1.0, 6.0, ((1, 4), (2, 8)), jnp.float32)
    reaction = jnp.clip(1.0 + 2.0 * jax.random.uniform(streams_of[2], (P_SIZE * P_SIZE, NEX, NEY), jnp.float32) ** block_scale(streams_of[2], (P_SIZE * P_SIZE, NEX, NEY), ((1, 4), (2, 8)), -0.2, 0.2), 1.0, 3.0)
    stiffness = jnp.clip(jnp.exp(math.log(2.0) - 1.3862944 * jax.random.uniform(streams_of[3], (NEX, NEY), jnp.float32) ** block_scale(streams_of[3], (NEX, NEY), ((0, 4), (1, 8)), -0.2, 0.2)), 0.5, 2.0)
    line_op = draw_line_op(jax.random.fold_in(streams_of[7], 71), 0)
    face_deriv = gaussian(streams_of[5], (P_SIZE,), 0.5, 2.0, (), jnp.float32)
    wall_flags = place_ends((jax.random.randint(streams_of[6], (4, NEX, NEY), 0, 4) < 1).astype(jnp.int32), jax.random.fold_in(streams_of[6], 1), 0, 1)
    return {"source": source, "initial": initial, "reaction": reaction, "stiffness": stiffness, "line_op": line_op, "face_deriv": face_deriv, "wall_flags": wall_flags}


TAU = 2.0
FLOOR = 0.1

def block_sum(values):
    flat = values.reshape(-1)
    width = 1024
    extra = -flat.shape[0] % width
    flat = jnp.concatenate([flat, jnp.zeros((extra,), flat.dtype)])
    return jnp.sum(lax.optimization_barrier(jnp.sum(flat.reshape(-1, width), axis=1)))

def apply_op(field, reaction, stiffness, line_op, face_deriv, wall_flags):
    highest = lax.Precision.HIGHEST
    nodes = field.reshape(P_SIZE, P_SIZE, field.shape[1], field.shape[2])
    interior = stiffness * (jnp.einsum('ac,cbxy->abxy', line_op, nodes, precision=highest) + jnp.einsum('bc,acxy->abxy', line_op, nodes, precision=highest))
    reversed_w = face_deriv[::-1]
    west_val = nodes[0]
    east_val = nodes[P_SIZE - 1]
    south_val = nodes[:, 0]
    north_val = nodes[:, P_SIZE - 1]
    west_der = jnp.einsum('c,cbxy->bxy', face_deriv, nodes, precision=highest)
    east_der = jnp.einsum('c,cbxy->bxy', reversed_w, nodes, precision=highest)
    south_der = jnp.einsum('c,acxy->axy', face_deriv, nodes, precision=highest)
    north_der = jnp.einsum('c,acxy->axy', reversed_w, nodes, precision=highest)
    opened = 1.0 - wall_flags.astype(field.dtype)
    add_east = TAU * (east_val - opened[1] * jnp.roll(west_val, -1, 1)) + 0.5 * (east_der - opened[1] * jnp.roll(west_der, -1, 1))
    add_west = TAU * (west_val - opened[0] * jnp.roll(east_val, 1, 1)) + 0.5 * (west_der - opened[0] * jnp.roll(east_der, 1, 1))
    add_north = TAU * (north_val - opened[3] * jnp.roll(south_val, -1, 2)) + 0.5 * (north_der - opened[3] * jnp.roll(south_der, -1, 2))
    add_south = TAU * (south_val - opened[2] * jnp.roll(north_val, 1, 2)) + 0.5 * (south_der - opened[2] * jnp.roll(north_der, 1, 2))
    result = reaction.reshape(nodes.shape) * nodes + interior
    result = result.at[0].add(add_west).at[P_SIZE - 1].add(add_east)
    result = result.at[:, 0].add(add_south).at[:, P_SIZE - 1].add(add_north)
    return result.reshape(field.shape)

def reference(source, initial, reaction, stiffness, line_op, face_deriv, wall_flags):
    total = float(P_SIZE * P_SIZE * NEX * NEY)

    def operate(field):
        return apply_op(field, reaction, stiffness, line_op, face_deriv, wall_flags)
    first = source - operate(initial)
    beta_first = jnp.sqrt(block_sum(first * first) / total + FLOOR)
    vectors = [first / beta_first]
    hessen = jnp.zeros((ITERS + 1, ITERS), source.dtype)
    for step in range(ITERS):
        image = operate(vectors[step])
        coeffs = [block_sum(vector * image) / total for vector in vectors]
        for index in range(len(vectors)):
            image = image - coeffs[index] * vectors[index]
            hessen = hessen.at[index, step].set(coeffs[index])
        beta = jnp.sqrt(block_sum(image * image) / total + FLOOR)
        hessen = hessen.at[step + 1, step].set(beta)
        vectors.append(image / beta)
    return (hessen, jnp.stack(vectors))
```

```python
import functools

import jax
import jax.numpy as jnp
from jax import lax
from jax.experimental import pallas as pl
from jax.experimental.pallas import tpu as pltpu
from jax.sharding import PartitionSpec as P

P_SIZE = 8
ITERS = 5
TAU = 2.0
FLOOR = 0.1
PAIRS = P_SIZE // 2
MESH = pl.DeviceIdType.MESH


def kernel(
    nx, ny, total,
    line, deriv, src, ini, rea, stf, wal,
    hess_out, basis_out,
    pend, image, bas, coef, gcoef, small,
    hsend, hrecv, rsend, rrecv,
    hs_sem, hr_sem, rs_sem, rr_sem, out_sem,
):
    n = nx * ny
    gx, gy = lax.axis_index("gx"), lax.axis_index("gy")
    me = gx * ny + gy

    def peer(k):
        t = lax.rem(me + k, n)
        return (t // ny, lax.rem(t, ny))

    east = (lax.rem(gx + 1, nx), gy)
    west = (lax.rem(gx + nx - 1, nx), gy)
    north = (gx, lax.rem(gy + 1, ny))
    south = (gx, lax.rem(gy + ny - 1, ny))

    barrier = pltpu.get_barrier_semaphore()

    def greet(k, carry):
        pl.semaphore_signal(barrier, inc=1, device_id=peer(k), device_id_type=MESH)
        return carry

    lax.fori_loop(1, n, greet, 0, unroll=n <= 64)

    sub = lax.broadcasted_iota(jnp.int32, (8, 128), 0)
    lane = lax.broadcasted_iota(jnp.int32, (8, 128), 1)
    low = sub < 4
    xpos = sub % 4

    def srl(v, s):
        s = s % 8
        return v if s == 0 else pltpu.roll(v, s, 0)

    def lrl(v, s):
        s = s % 128
        return v if s == 0 else pltpu.roll(v, s, 1)

    def halves(a, b):
        return jnp.where(low, a, b)

    for p in range(PAIRS):
        for r in range(PAIRS):
            coef[(p * PAIRS + r) * 2] = halves(line[2 * p, 2 * r], line[2 * p + 1, 2 * r + 1])
            coef[(p * PAIRS + r) * 2 + 1] = halves(line[2 * p, 2 * r + 1], line[2 * p + 1, 2 * r])
    glow = [0.5 * deriv[c] + (TAU if c == 0 else 0.0) for c in range(P_SIZE)]
    gupp = [
        0.5 * deriv[P_SIZE - 1 - c] + (TAU if c == P_SIZE - 1 else 0.0) for c in range(P_SIZE)
    ]
    for p in range(PAIRS):
        gcoef[p] = halves(glow[2 * p], glow[2 * p + 1])
        gcoef[PAIRS + p] = halves(gupp[2 * p], gupp[2 * p + 1])
    small[0, 0:4] = stf[...]
    small[0, 4:8] = stf[...]
    opened = [1.0 - wal[f].astype(jnp.float32) for f in range(4)]
    for slot, (first, second) in enumerate(((0, 0), (1, 1), (2, 3))):
        small[slot + 1, 0:4] = opened[first]
        small[slot + 1, 4:8] = opened[second]

    def tile(ref, a, p):
        return ref[pl.ds((a * PAIRS + p) * 8, 8), :]

    def put(ref, a, p, value):
        ref[pl.ds((a * PAIRS + p) * 8, 8), :] = value

    def xfaces(get):
        fw, fe = [], []
        for p in range(PAIRS):
            w = e = None
            for c in range(P_SIZE):
                v = get(c, p)
                w = glow[c] * v if w is None else w + glow[c] * v
                e = gupp[c] * v if e is None else e + gupp[c] * v
            fw.append(w)
            fe.append(e)
        return fw, fe

    def yfaces(get):
        own, across = [], []
        for a in range(P_SIZE):
            s = t = None
            for p in range(PAIRS):
                v = get(a, p)
                s = gcoef[p] * v if s is None else s + gcoef[p] * v
                t = gcoef[PAIRS + p] * v if t is None else t + gcoef[PAIRS + p] * v
            u = halves(s, t) + srl(halves(t, s), 4)
            q = srl(u, 4)
            own.append(u)
            across.append(halves(lrl(q, 1), lrl(q, 127)))
        return own, across

    def send_halo(slot, get):
        fw, fe = xfaces(get)
        cw, ce = fw[0], srl(fe[0], -3)
        for p in range(1, PAIRS):
            cw = jnp.where(xpos == p, srl(fw[p], p), cw)
            ce = jnp.where(xpos == p, srl(fe[p], p - 3), ce)
        hsend[slot, 0] = cw
        hsend[slot, 1] = ce
        copies = [halo_copy(slot, 0, 0, west), halo_copy(slot, 1, 1, east)]
        for copy in copies:
            copy.start()
        own, across = yfaces(get)
        packed = across[0]
        for a in range(1, P_SIZE):
            mask = lane == jnp.where(low, a, a - 1)
            packed = jnp.where(mask, lrl(across[a], a), packed)
        hsend[slot, 2] = packed
        more = [halo_copy(slot, 2, 2, north), halo_copy(slot, 2, 3, south)]
        for copy in more:
            copy.start()
        return copies + more, (fw, fe, own, across)

    def halo_copy(slot, source, target, device):
        return pltpu.make_async_remote_copy(
            src_ref=hsend.at[slot, source],
            dst_ref=hrecv.at[slot, target],
            send_sem=hs_sem.at[slot, target],
            recv_sem=hr_sem.at[slot, target],
            device_id=device,
            device_id_type=MESH,
        )

    def take_halo(slot, copies):
        for copy in copies:
            copy.wait_recv()
        return (
            hrecv[slot, 0],
            hrecv[slot, 1],
            halves(hrecv[slot, 2], hrecv[slot, 3]),
        )

    edge = lane == jnp.where(low, 0, 127)

    def operate(get, halo, faces, emit):
        fw, fe, own, across = faces
        cw, ce, cy = halo
        stiff, open_w, open_e, open_y = small[0], small[1], small[2], small[3]
        sides = {}
        for p in range(PAIRS):
            nb_e = jnp.where(xpos == 3, srl(cw, 3 - p), srl(fw[p], 7))
            nb_w = jnp.where(xpos == 0, srl(ce, -p), srl(fe[p], 1))
            sides[0, p] = fw[p] - open_w * nb_w
            sides[P_SIZE - 1, p] = fe[p] - open_e * nb_e
        for a in range(P_SIZE):
            nb = jnp.where(edge, lrl(cy, -a), across[a])
            term = own[a] - open_y * nb
            vs = [get(a, p) for p in range(PAIRS)]
            ss = [srl(v, 4) for v in vs]
            for p in range(PAIRS):
                acc = None
                for r in range(PAIRS):
                    k = (p * PAIRS + r) * 2
                    part = coef[k] * vs[r] + coef[k + 1] * ss[r]
                    acc = part if acc is None else acc + part
                other = None
                for c in range(P_SIZE):
                    part = line[a, c] * get(c, p)
                    other = part if other is None else other + part
                value = tile(rea, a, p) * vs[p] + stiff * (acc + other)
                if p == 0:
                    value = value + jnp.where(low, term, 0.0)
                if p == PAIRS - 1:
                    value = value + jnp.where(low, 0.0, term)
                if (a, p) in sides:
                    value = value + sides[a, p]
                emit(a, p, value)

    def faces_of(get):
        fw, fe = xfaces(get)
        own, across = yfaces(get)
        return fw, fe, own, across

    def gather_rows(accs):
        zero = jnp.zeros((8, 128), jnp.float32)
        level = list(accs) + [zero] * (8 - len(accs))
        for shift in (1, 2, 4):
            keep = (sub // shift) % 2 == 0
            level = [
                jnp.where(keep, level[i], level[i + 1])
                + srl(jnp.where(keep, level[i + 1], level[i]), shift)
                for i in range(0, len(level), 2)
            ]
        return level[0]

    def fold(v):
        for shift in (4, 2, 1):
            v = v + srl(v, shift)
        return v

    def row_copy(slot, k):
        return pltpu.make_async_remote_copy(
            src_ref=rsend.at[slot],
            dst_ref=rrecv.at[slot, pl.ds(me, 1)],
            send_sem=rs_sem.at[slot],
            recv_sem=rr_sem.at[slot],
            device_id=peer(k),
            device_id_type=MESH,
        )

    def start_reduce(slot, accs):
        packed = None
        for start in range(0, len(accs), 8):
            sums = jnp.sum(gather_rows(accs[start:start + 8]), axis=1, keepdims=True)
            part = jnp.where(lane == sub + start, sums, 0.0)
            packed = part if packed is None else packed + part
        row = fold(packed)[0:1]
        rsend[slot] = row
        rrecv[slot, pl.ds(me, 1)] = row

        def push(k, carry):
            row_copy(slot, k).start()
            return carry

        lax.fori_loop(1, n, push, 0, unroll=n <= 64)

    def end_reduce(slot, count):
        block = rrecv.at[slot, pl.ds(0, n - 1)]
        pltpu.make_async_copy(block, block, rr_sem.at[slot]).wait()
        value = rrecv[slot, 0:8]
        for g in range(1, n // 8):
            value = value + rrecv[slot, 8 * g:8 * g + 8]
        value = fold(value)
        return [jnp.broadcast_to(value[:, k:k + 1], (8, 128)) for k in range(count)]

    get_ini = functools.partial(tile, ini)
    get_pend = functools.partial(tile, pend)
    get_image = functools.partial(tile, image)

    pl.semaphore_wait(barrier, n - 1)
    started = []
    copies, faces = send_halo(0, get_ini)
    started += copies
    halo = take_halo(0, copies)
    operate(get_ini, halo, faces, lambda a, p, v: put(pend, a, p, tile(src, a, p) - v))

    copies, faces = send_halo(1, get_pend)
    started += copies
    halo = take_halo(1, copies)

    hess = jnp.zeros((8, 128), jnp.float32)
    halos, written = [], []
    gram = {}
    for step in range(ITERS):
        last = step == ITERS - 1
        operate(get_pend, halo, faces, functools.partial(put, image))
        if not last:
            copies, _ = send_halo(step + 2, get_image)
            started += copies
        accs = [None] * (2 * step + 2 + (1 if last else 0))
        for a in range(P_SIZE):
            for p in range(PAIRS):
                w, v = get_image(a, p), get_pend(a, p)
                terms = [w * v, v * v]
                for i in range(step):
                    b = bas[i, pl.ds((a * PAIRS + p) * 8, 8), :]
                    terms += [b * w, b * v]
                if last:
                    terms.append(w * w)
                accs = [t if s is None else s + t for s, t in zip(accs, terms)]
        start_reduce(step, accs)
        sums = end_reduce(step, len(accs))
        beta = jnp.sqrt(sums[1] / total + FLOOR)
        inv = 1.0 / beta
        scaled = inv / total
        coeffs = [sums[2 + 2 * i] * scaled for i in range(step)] + [sums[0] * scaled * inv]
        for i in range(step):
            gram[i, step] = sums[3 + 2 * i] * scaled
        gram[step, step] = sums[1] * scaled * inv
        for i in range(step + 1):
            hess = jnp.where((sub == i) & (lane == step), coeffs[i], hess)
        if step:
            hess = jnp.where((sub == step) & (lane == step - 1), beta, hess)
        if last:
            square = sums[-1] * scaled * inv
            for i in range(ITERS):
                inner = None
                for k in range(ITERS):
                    g = gram[min(i, k), max(i, k)] * coeffs[k]
                    inner = g if inner is None else inner + g
                square = square + coeffs[i] * (inner - 2.0 * coeffs[i])
            final = jnp.sqrt(jnp.maximum(square, 0.0) + FLOOR)
            hess = jnp.where((sub == ITERS) & (lane == ITERS - 1), final, hess)
            post = 1.0 / final
        for a in range(P_SIZE):
            for p in range(PAIRS):
                b = get_pend(a, p) * inv
                bas[step, pl.ds((a * PAIRS + p) * 8, 8), :] = b
                v = get_image(a, p) * inv - coeffs[step] * b
                for i in range(step):
                    v = v - coeffs[i] * bas[i, pl.ds((a * PAIRS + p) * 8, 8), :]
                if last:
                    bas[ITERS, pl.ds((a * PAIRS + p) * 8, 8), :] = v * post
                else:
                    put(pend, a, p, v)
        out = pltpu.make_async_copy(bas.at[step], basis_out.at[step], out_sem.at[step])
        out.start()
        written.append(out)
        if not last:
            halos.append([h * inv for h in halo])
            fresh = take_halo(step + 2, copies)
            nxt = []
            for k in range(3):
                h = fresh[k] * inv
                for i in range(step + 1):
                    h = h - coeffs[i] * halos[i][k]
                nxt.append(h)
            halo = nxt
            faces = faces_of(get_pend)
    out = pltpu.make_async_copy(bas.at[ITERS], basis_out.at[ITERS], out_sem.at[ITERS])
    out.start()
    hess_out[...] = hess[0:ITERS + 1, 0:ITERS]
    for copy in started:
        copy.wait_send()
    for slot in range(ITERS):
        block = rrecv.at[slot, pl.ds(0, n - 1)]
        pltpu.make_async_copy(block, block, rs_sem.at[slot]).wait()
    for copy in written + [out]:
        copy.wait()


def body(nx, ny, source, initial, reaction, stiffness, line_op, face_deriv, wall_flags):
    nodes, ex, ey = source.shape
    n = nx * ny
    rows = nodes * ex
    flat = (rows, ey)
    total = float(nodes * ex * nx * ey * ny)
    vmem = pl.BlockSpec(memory_space=pltpu.VMEM)
    smem = pl.BlockSpec(memory_space=pltpu.SMEM)
    hess, basis = pl.pallas_call(
        functools.partial(kernel, nx, ny, total),
        out_shape=(
            jax.ShapeDtypeStruct((ITERS + 1, ITERS), jnp.float32),
            jax.ShapeDtypeStruct((ITERS + 1,) + flat, jnp.float32),
        ),
        in_specs=[smem, smem, vmem, vmem, vmem, vmem, vmem],
        out_specs=(vmem, pl.BlockSpec(memory_space=pl.ANY)),
        scratch_shapes=[
            pltpu.VMEM(flat, jnp.float32),
            pltpu.VMEM(flat, jnp.float32),
            pltpu.VMEM((ITERS + 1,) + flat, jnp.float32),
            pltpu.VMEM((2 * PAIRS * PAIRS, 8, 128), jnp.float32),
            pltpu.VMEM((2 * PAIRS, 8, 128), jnp.float32),
            pltpu.VMEM((4, 8, 128), jnp.float32),
            pltpu.VMEM((ITERS + 1, 3, 8, 128), jnp.float32),
            pltpu.VMEM((ITERS + 1, 4, 8, 128), jnp.float32),
            pltpu.VMEM((ITERS, 1, 128), jnp.float32),
            pltpu.VMEM((ITERS, n, 128), jnp.float32),
            pltpu.SemaphoreType.DMA((ITERS + 1, 4)),
            pltpu.SemaphoreType.DMA((ITERS + 1, 4)),
            pltpu.SemaphoreType.DMA((ITERS,)),
            pltpu.SemaphoreType.DMA((ITERS,)),
            pltpu.SemaphoreType.DMA((ITERS + 1,)),
        ],
        compiler_params=pltpu.CompilerParams(collective_id=0, has_side_effects=True),
    )(
        line_op, face_deriv, source.reshape(flat), initial.reshape(flat), reaction.reshape(flat),
        stiffness, wall_flags,
    )
    return hess, basis.reshape((ITERS + 1, nodes, ex, ey))


def solution(mesh):
    return jax.shard_map(
        functools.partial(body, mesh.shape["gx"], mesh.shape["gy"]),
        mesh=mesh,
        in_specs=(
            P(None, "gx", "gy"),
            P(None, "gx", "gy"),
            P(None, "gx", "gy"),
            P("gx", "gy"),
            P(),
            P(),
            P(None, "gx", "gy"),
        ),
        out_specs=(P(), P(None, None, "gx", "gy")),
        check_vma=False,
    )
```

```python
import functools

import jax
import jax.numpy as jnp
from jax import lax
from jax.experimental import pallas as pl
from jax.experimental.pallas import tpu as pltpu
from jax.sharding import PartitionSpec as P

P_SIZE = 8
ITERS = 5
TAU = 2.0
FLOOR = 0.1
PAIRS = P_SIZE // 2
MESH = pl.DeviceIdType.MESH


def kernel(
    nx, ny, total,
    line, deriv, src_any, ini_any, rea_any, stf, wal,
    hess_out, bas,
    pend, image, coef, gcoef, small, src, ini, rea, in_sem,
    hsend, hrecv, rsend, rrecv,
    hs_sem, hr_sem, rs_sem, rr_sem,
):
    n = nx * ny
    gx, gy = lax.axis_index("gx"), lax.axis_index("gy")
    me = gx * ny + gy

    side = gy // (ny // 2)
    offsets = sorted(range(1, nx), key=lambda d: abs(2 * d - nx))

    def for_peers(act):
        def column(k, own_column):
            across = side * k + (1 - side) * (ny - 1 - k)
            for d in offsets:
                act((lax.rem(gx + d, nx), across))
            if own_column:
                skip = jnp.where(k >= (side * gy + (1 - side) * (ny - 1 - gy)), 1, 0)
                act((gx, across + (2 * side - 1) * skip))

        if n <= 64:
            for k in range(ny - 1):
                column(k, True)
        else:
            lax.fori_loop(0, ny - 1, lambda k, c: (column(k, True), c)[1], 0)
        column(ny - 1, False)

    east = (lax.rem(gx + 1, nx), gy)
    west = (lax.rem(gx + nx - 1, nx), gy)
    north = (gx, lax.rem(gy + 1, ny))
    south = (gx, lax.rem(gy + ny - 1, ny))

    barrier = pltpu.get_barrier_semaphore()

    def greet(device):
        pl.semaphore_signal(barrier, inc=1, device_id=device, device_id_type=MESH)

    loads = [
        pltpu.make_async_copy(given, held, in_sem.at[k])
        for k, (given, held) in enumerate(((ini_any, ini), (src_any, src), (rea_any, rea)))
    ]
    for load in loads:
        load.start()
    for_peers(greet)

    sub = lax.broadcasted_iota(jnp.int32, (8, 128), 0)
    lane = lax.broadcasted_iota(jnp.int32, (8, 128), 1)
    low = sub < 4
    xpos = sub % 4

    def srl(v, s):
        s = s % 8
        return v if s == 0 else pltpu.roll(v, s, 0)

    def lrl(v, s):
        s = s % 128
        return v if s == 0 else pltpu.roll(v, s, 1)

    def halves(a, b):
        return jnp.where(low, a, b)

    for p in range(PAIRS):
        for r in range(PAIRS):
            coef[(p * PAIRS + r) * 2] = halves(line[2 * p, 2 * r], line[2 * p + 1, 2 * r + 1])
            coef[(p * PAIRS + r) * 2 + 1] = halves(line[2 * p, 2 * r + 1], line[2 * p + 1, 2 * r])
    glow = [0.5 * deriv[c] + (TAU if c == 0 else 0.0) for c in range(P_SIZE)]
    gupp = [
        0.5 * deriv[P_SIZE - 1 - c] + (TAU if c == P_SIZE - 1 else 0.0) for c in range(P_SIZE)
    ]
    for p in range(PAIRS):
        gcoef[p] = halves(glow[2 * p], glow[2 * p + 1])
        gcoef[PAIRS + p] = halves(gupp[2 * p], gupp[2 * p + 1])
    small[0, 0:4] = stf[...]
    small[0, 4:8] = stf[...]
    opened = [1.0 - wal[f].astype(jnp.float32) for f in range(4)]
    for slot, (first, second) in enumerate(((0, 0), (1, 1), (2, 3))):
        small[slot + 1, 0:4] = opened[first]
        small[slot + 1, 4:8] = opened[second]

    def tile(ref, a, p):
        return ref[pl.ds((a * PAIRS + p) * 8, 8), :]

    def put(ref, a, p, value):
        ref[pl.ds((a * PAIRS + p) * 8, 8), :] = value

    def xfaces(get):
        fw, fe = [], []
        for p in range(PAIRS):
            w = e = None
            for c in range(P_SIZE):
                v = get(c, p)
                w = glow[c] * v if w is None else w + glow[c] * v
                e = gupp[c] * v if e is None else e + gupp[c] * v
            fw.append(w)
            fe.append(e)
        return fw, fe

    def yfaces(get):
        own, across = [], []
        for a in range(P_SIZE):
            s = t = None
            for p in range(PAIRS):
                v = get(a, p)
                s = gcoef[p] * v if s is None else s + gcoef[p] * v
                t = gcoef[PAIRS + p] * v if t is None else t + gcoef[PAIRS + p] * v
            u = halves(s, t) + srl(halves(t, s), 4)
            q = srl(u, 4)
            own.append(u)
            across.append(halves(lrl(q, 1), lrl(q, 127)))
        return own, across

    def send_halo(slot, get, ready=lambda: None):
        fw, fe = xfaces(get)
        cw, ce = fw[0], srl(fe[0], -3)
        for p in range(1, PAIRS):
            cw = jnp.where(xpos == p, srl(fw[p], p), cw)
            ce = jnp.where(xpos == p, srl(fe[p], p - 3), ce)
        hsend[slot, 0] = cw
        hsend[slot, 1] = ce
        own, across = yfaces(get)
        packed = across[0]
        for a in range(1, P_SIZE):
            mask = lane == jnp.where(low, a, a - 1)
            packed = jnp.where(mask, lrl(across[a], a), packed)
        hsend[slot, 2] = packed
        ready()
        copies = [
            halo_copy(slot, 2, 2, north), halo_copy(slot, 2, 3, south),
            halo_copy(slot, 0, 0, west), halo_copy(slot, 1, 1, east),
        ]
        for copy in copies:
            copy.start()
        return copies, (fw, fe, own, across)

    def halo_copy(slot, source, target, device):
        return pltpu.make_async_remote_copy(
            src_ref=hsend.at[slot, source],
            dst_ref=hrecv.at[slot, target],
            send_sem=hs_sem.at[slot, target],
            recv_sem=hr_sem.at[slot, target],
            device_id=device,
            device_id_type=MESH,
        )

    def take_halo(slot, copies):
        for copy in copies:
            copy.wait_recv()
        return (
            hrecv[slot, 0],
            hrecv[slot, 1],
            halves(hrecv[slot, 2], hrecv[slot, 3]),
        )

    edge = lane == jnp.where(low, 0, 127)

    def operate(get, halo, faces, emit):
        fw, fe, own, across = faces
        cw, ce, cy = halo
        stiff, open_w, open_e, open_y = small[0], small[1], small[2], small[3]
        sides = {}
        for p in range(PAIRS):
            nb_e = jnp.where(xpos == 3, srl(cw, 3 - p), srl(fw[p], 7))
            nb_w = jnp.where(xpos == 0, srl(ce, -p), srl(fe[p], 1))
            sides[0, p] = fw[p] - open_w * nb_w
            sides[P_SIZE - 1, p] = fe[p] - open_e * nb_e
        for a in range(P_SIZE):
            nb = jnp.where(edge, lrl(cy, -a), across[a])
            term = own[a] - open_y * nb
            vs = [get(a, p) for p in range(PAIRS)]
            ss = [srl(v, 4) for v in vs]
            for p in range(PAIRS):
                acc = None
                for r in range(PAIRS):
                    k = (p * PAIRS + r) * 2
                    part = coef[k] * vs[r] + coef[k + 1] * ss[r]
                    acc = part if acc is None else acc + part
                other = None
                for c in range(P_SIZE):
                    part = line[a, c] * get(c, p)
                    other = part if other is None else other + part
                value = tile(rea, a, p) * vs[p] + stiff * (acc + other)
                if p == 0:
                    value = value + jnp.where(low, term, 0.0)
                if p == PAIRS - 1:
                    value = value + jnp.where(low, 0.0, term)
                if (a, p) in sides:
                    value = value + sides[a, p]
                emit(a, p, value)

    def faces_of(get):
        fw, fe = xfaces(get)
        own, across = yfaces(get)
        return fw, fe, own, across

    def gather_rows(accs):
        zero = jnp.zeros((8, 128), jnp.float32)
        level = list(accs) + [zero] * (8 - len(accs))
        for shift in (1, 2, 4):
            keep = (sub // shift) % 2 == 0
            level = [
                jnp.where(keep, level[i], level[i + 1])
                + srl(jnp.where(keep, level[i + 1], level[i]), shift)
                for i in range(0, len(level), 2)
            ]
        return level[0]

    def fold(v):
        for shift in (4, 2, 1):
            v = v + srl(v, shift)
        return v

    def row_copy(slot, device):
        return pltpu.make_async_remote_copy(
            src_ref=rsend.at[slot],
            dst_ref=rrecv.at[slot, pl.ds(me, 1)],
            send_sem=rs_sem.at[slot],
            recv_sem=rr_sem.at[slot],
            device_id=device,
            device_id_type=MESH,
        )

    def start_reduce(slot, accs):
        packed = None
        for start in range(0, len(accs), 8):
            sums = jnp.sum(gather_rows(accs[start:start + 8]), axis=1, keepdims=True)
            part = jnp.where(lane == sub + start, sums, 0.0)
            packed = part if packed is None else packed + part
        row = fold(packed)[0:1]
        rsend[slot] = row
        rrecv[slot, pl.ds(me, 1)] = row

        for_peers(lambda device: row_copy(slot, device).start())

    def end_reduce(slot, count):
        block = rrecv.at[slot, pl.ds(0, n - 1)]
        pltpu.make_async_copy(block, block, rr_sem.at[slot]).wait()
        value = rrecv[slot, 0:8]
        for g in range(1, n // 8):
            value = value + rrecv[slot, 8 * g:8 * g + 8]
        value = fold(value)
        return [jnp.broadcast_to(value[:, k:k + 1], (8, 128)) for k in range(count)]

    get_ini = functools.partial(tile, ini)
    get_pend = functools.partial(tile, pend)
    get_image = functools.partial(tile, image)

    started = []
    loads[0].wait()
    copies, faces = send_halo(0, get_ini, lambda: pl.semaphore_wait(barrier, n - 1))
    loads[1].wait()
    loads[2].wait()
    started += copies
    halo = take_halo(0, copies)
    operate(get_ini, halo, faces, lambda a, p, v: put(pend, a, p, tile(src, a, p) - v))

    copies, faces = send_halo(1, get_pend)
    started += copies
    halo = take_halo(1, copies)

    hess = jnp.zeros((8, 128), jnp.float32)
    halos = []
    gram = {}
    for step in range(ITERS):
        last = step == ITERS - 1
        operate(get_pend, halo, faces, functools.partial(put, image))
        if not last:
            copies, _ = send_halo(step + 2, get_image)
            started += copies
        accs = [None] * (2 * step + 2 + (1 if last else 0))
        for a in range(P_SIZE):
            for p in range(PAIRS):
                w, v = get_image(a, p), get_pend(a, p)
                terms = [w * v, v * v]
                for i in range(step):
                    b = bas[i, pl.ds((a * PAIRS + p) * 8, 8), :]
                    terms += [b * w, b * v]
                if last:
                    terms.append(w * w)
                accs = [t if s is None else s + t for s, t in zip(accs, terms)]
        start_reduce(step, accs)
        sums = end_reduce(step, len(accs))
        beta = jnp.sqrt(sums[1] / total + FLOOR)
        inv = 1.0 / beta
        scaled = inv / total
        coeffs = [sums[2 + 2 * i] * scaled for i in range(step)] + [sums[0] * scaled * inv]
        for i in range(step):
            gram[i, step] = sums[3 + 2 * i] * scaled
        gram[step, step] = sums[1] * scaled * inv
        for i in range(step + 1):
            hess = jnp.where((sub == i) & (lane == step), coeffs[i], hess)
        if step:
            hess = jnp.where((sub == step) & (lane == step - 1), beta, hess)
        if last:
            square = sums[-1] * scaled * inv
            for i in range(ITERS):
                inner = None
                for k in range(ITERS):
                    g = gram[min(i, k), max(i, k)] * coeffs[k]
                    inner = g if inner is None else inner + g
                square = square + coeffs[i] * (inner - 2.0 * coeffs[i])
            final = jnp.sqrt(jnp.maximum(square, 0.0) + FLOOR)
            hess = jnp.where((sub == ITERS) & (lane == ITERS - 1), final, hess)
            post = 1.0 / final
        for a in range(P_SIZE):
            for p in range(PAIRS):
                b = get_pend(a, p) * inv
                bas[step, pl.ds((a * PAIRS + p) * 8, 8), :] = b
                v = get_image(a, p) * inv - coeffs[step] * b
                for i in range(step):
                    v = v - coeffs[i] * bas[i, pl.ds((a * PAIRS + p) * 8, 8), :]
                if last:
                    bas[ITERS, pl.ds((a * PAIRS + p) * 8, 8), :] = v * post
                else:
                    put(pend, a, p, v)
        if not last:
            halos.append([h * inv for h in halo])
            fresh = take_halo(step + 2, copies)
            nxt = []
            for k in range(3):
                h = fresh[k] * inv
                for i in range(step + 1):
                    h = h - coeffs[i] * halos[i][k]
                nxt.append(h)
            halo = nxt
            faces = faces_of(get_pend)
    hess_out[...] = hess[0:ITERS + 1, 0:ITERS]
    for copy in started:
        copy.wait_send()
    for slot in range(ITERS):
        block = rrecv.at[slot, pl.ds(0, n - 1)]
        pltpu.make_async_copy(block, block, rs_sem.at[slot]).wait()


def store(hess, basis, hess_out, basis_out, sem):
    copies = [
        pltpu.make_async_copy(basis, basis_out, sem.at[0]),
        pltpu.make_async_copy(hess, hess_out, sem.at[1]),
    ]
    for copy in copies:
        copy.start()
    for copy in copies:
        copy.wait()


def body(nx, ny, source, initial, reaction, stiffness, line_op, face_deriv, wall_flags):
    nodes, ex, ey = source.shape
    n = nx * ny
    rows = nodes * ex
    flat = (rows, ey)
    total = float(nodes * ex * nx * ey * ny)
    vmem = pl.BlockSpec(memory_space=pltpu.VMEM)
    hbm = pl.BlockSpec(memory_space=pl.ANY)
    smem = pl.BlockSpec(memory_space=pltpu.SMEM)
    hess, basis = pl.pallas_call(
        functools.partial(kernel, nx, ny, total),
        out_shape=(
            pltpu.VMEM((ITERS + 1, ITERS), jnp.float32),
            pltpu.VMEM((ITERS + 1,) + flat, jnp.float32),
        ),
        in_specs=[smem, smem, hbm, hbm, hbm, vmem, vmem],
        out_specs=(vmem, vmem),
        scratch_shapes=[
            pltpu.VMEM(flat, jnp.float32),
            pltpu.VMEM(flat, jnp.float32),
            pltpu.VMEM((2 * PAIRS * PAIRS, 8, 128), jnp.float32),
            pltpu.VMEM((2 * PAIRS, 8, 128), jnp.float32),
            pltpu.VMEM((4, 8, 128), jnp.float32),
            pltpu.VMEM(flat, jnp.float32),
            pltpu.VMEM(flat, jnp.float32),
            pltpu.VMEM(flat, jnp.float32),
            pltpu.SemaphoreType.DMA((3,)),
            pltpu.VMEM((ITERS + 1, 3, 8, 128), jnp.float32),
            pltpu.VMEM((ITERS + 1, 4, 8, 128), jnp.float32),
            pltpu.VMEM((ITERS, 1, 128), jnp.float32),
            pltpu.VMEM((ITERS, n, 128), jnp.float32),
            pltpu.SemaphoreType.DMA((ITERS + 1, 4)),
            pltpu.SemaphoreType.DMA((ITERS + 1, 4)),
            pltpu.SemaphoreType.DMA((ITERS,)),
            pltpu.SemaphoreType.DMA((ITERS,)),
        ],
        compiler_params=pltpu.CompilerParams(collective_id=0, has_side_effects=True),
    )(
        line_op, face_deriv, source.reshape(flat), initial.reshape(flat), reaction.reshape(flat),
        stiffness, wall_flags,
    )
    hess = pltpu.with_memory_space_constraint(hess, pltpu.VMEM)
    basis = pltpu.with_memory_space_constraint(basis, pltpu.VMEM)
    hess, basis = pl.pallas_call(
        store,
        out_shape=(
            jax.ShapeDtypeStruct(hess.shape, jnp.float32),
            jax.ShapeDtypeStruct(basis.shape, jnp.float32),
        ),
        in_specs=[hbm, hbm],
        out_specs=(hbm, hbm),
        scratch_shapes=[pltpu.SemaphoreType.DMA((2,))],
    )(hess, basis)
    return hess, basis.reshape((ITERS + 1, nodes, ex, ey))


def solution(mesh):
    return jax.shard_map(
        functools.partial(body, mesh.shape["gx"], mesh.shape["gy"]),
        mesh=mesh,
        in_specs=(
            P(None, "gx", "gy"),
            P(None, "gx", "gy"),
            P(None, "gx", "gy"),
            P("gx", "gy"),
            P(),
            P(),
            P(None, "gx", "gy"),
        ),
        out_specs=(P(), P(None, None, "gx", "gy")),
        check_vma=False,
    )
```
